256 devices in a mesh: cluster: 8 (over z), member: 32 (over y, x, core).
Axes of the slice: x: 4, y: 4, z: 8, core: 2. Of those that a mesh axis runs over, the one named last changes fastest.
Arguments:
- factors: float32 [512, 1024, 1024], P(('cluster', 'member')), as said below
- panels: float32 [512, 1024, 256], P(('cluster', 'member')), may hold values from -0.046875 to 0.046875
- sizes: int32 [512], P(('cluster', 'member')), may hold values from 512 to 1024
- glue_index: int32 [512, 256], P(('cluster', 'member')), may hold values from 0 to 1023, as said below
- loads: float32 [8192, 256], P(('cluster', 'member')), may hold values from -6 to 6
Outputs:
- dual_rows: float32 [8192, 1024], P(('cluster', 'member'))
- products: float32 [8192, 256], P(('cluster', 'member'))
The draws below stay inside these ranges and needn't reach their ends.
Inputs may be any that keep to these rules, and one draw needn't show every extreme that they name: `glue_index`: the 256 entries of one subdomain are distinct; at most 16 of them lie in any one aligned block of 1024 // 32 dual rows, and every subdomain has 16 in some block. `factors`: strictly upper entries are zero; diagonal entries positive.
All inputs are finite; a program needn't handle non-finite values.
Results may differ from the reference program's by a relative error of at most 0.0003.
Values sent between devices are 32-bit elements; how exact they have to be, the bound alone decides.
A program may use at most 192 MiB of HBM per device.

```python
import math
import jax
import jax.numpy as jnp
from jax import lax

ORDER = 1024
PANEL = 256
NDUAL = 1024
IFACE = 8
SUB_DEV = 2
NRHS = 256
SUBS = 512
ALLDUAL = 8192
N_CLUSTER = 8
N_MEMBER = 32


def draw_factors(key, part):
    key_diag, key_lower = jax.random.split(key)
    diagonal = jax.random.uniform(key_diag, (SUBS, ORDER), jnp.float32, 1.0, 2.0)
    lower_part = 0.4 * jax.random.normal(key_lower, (SUBS, ORDER, ORDER), jnp.float32) / math.sqrt(ORDER)
    strict = jnp.tril(lower_part, -1)
    return strict + diagonal[:, :, None] * jnp.eye(ORDER, dtype=jnp.float32)


def draw_glue_index(key, part):
    row_share = NDUAL // N_MEMBER
    capacity = 2 * PANEL // N_MEMBER
    pair_count = N_MEMBER // 2
    key_split, key_order, key_rank, key_pick = jax.random.split(jax.random.fold_in(key, 7), 4)
    first_share = jax.random.randint(key_split, (SUBS, pair_count), 0, capacity + 1)
    first_share = first_share.at[:, 0].set(capacity)
    paired = jnp.stack([first_share, capacity - first_share], axis=-1).reshape(SUBS, N_MEMBER)
    order_keys = jax.random.split(key_order, SUBS)
    block_order = jax.vmap(lambda one_key: jax.random.permutation(one_key, N_MEMBER))(order_keys).astype(jnp.int32)
    inverse = jnp.argsort(block_order, axis=1).astype(jnp.int32)
    counts = jnp.take_along_axis(paired, inverse, axis=1)
    scores = jax.random.randint(key_rank, (SUBS, N_MEMBER, row_share), 0, 2 ** 20) * row_share
    scores = scores + lax.broadcasted_iota(jnp.int32, (SUBS, N_MEMBER, row_share), 2)
    ranks = jnp.argsort(jnp.argsort(scores, axis=2), axis=2).astype(jnp.int32)
    chosen = (ranks < counts[:, :, None]).reshape(SUBS, NDUAL)
    picking = jax.random.randint(key_pick, (SUBS, NDUAL), 0, 2 ** 19) * NDUAL
    picking = picking + lax.broadcasted_iota(jnp.int32, (SUBS, NDUAL), 1)
    ordering = jnp.where(chosen, 0, 2 ** 30).astype(jnp.int32) + picking
    return jnp.argsort(ordering, axis=1)[:, :PANEL].astype(jnp.int32)


def touch_ends(drawn, rng, smallest, high):
    longest = drawn.shape.index(max(drawn.shape))
    spots = []
    for shift in (0, 1):
        where = [jax.random.randint(jax.random.fold_in(rng, axis), (), 0, length) for axis, length in enumerate(drawn.shape)]
        where[longest] = (where[longest] + shift) % drawn.shape[longest]
        spots.append(tuple(where))
    return drawn.at[spots[0]].set(smallest).at[spots[1]].set(high)


def shard_levels(stream_key, extent, pieces, least, largest):
    loudness = 1.0
    for dim, blocks in pieces:
        draws = jax.random.uniform(jax.random.fold_in(jax.random.fold_in(stream_key, 6), dim), (blocks,), jnp.float32, least / len(pieces), largest / len(pieces))
        loudness = loudness * jnp.repeat(jnp.exp(draws), extent[dim] // blocks).reshape((-1,) + (1,) * (len(extent) - 1 - dim))
    return loudness


def bell_draw(stream_key, extent, deviation, limit, shards=(), held_as=jnp.bfloat16):
    values = jax.random.normal(stream_key, extent, jnp.float32) * deviation
    if len(shards) > 0:
        values = shard_levels(stream_key, extent, shards, -0.22, 0.18) * values
    return jnp.clip(values, min=-limit, max=limit).astype(held_as)


def setup_inputs(seed: int = 0) -> dict:
    key_of = jax.random.split(jax.random.key(seed), 6)
    return {
        "factors": draw_factors(jax.random.fold_in(key_of[5], 71), 0),
        "panels": bell_draw(key_of[1], (SUBS, ORDER, PANEL), (ORDER * SUB_DEV * N_MEMBER * PANEL // NDUAL) ** -0.5, 0.046875, ((0, 256),), jnp.float32),
        "sizes": touch_ends(jax.random.randint(key_of[2], (SUBS,), ORDER // 2, ORDER + 1), jax.random.fold_in(key_of[2], 1), ORDER // 2, ORDER).astype(jnp.int32),
        "glue_index": draw_glue_index(jax.random.fold_in(key_of[5], 71), 0),
        "loads": bell_draw(key_of[4], (ALLDUAL, NRHS), 1.0, 6.0, ((0, 256),), jnp.float32),
    }


def one_subdomain(items):
    factor, gluing, live_size = items
    factor_order = factor.shape[0]
    row_ids = lax.broadcasted_iota(jnp.int32, (factor_order, factor_order), 0)
    col_ids = lax.broadcasted_iota(jnp.int32, (factor_order, factor_order), 1)
    keeping = (row_ids < live_size) & (col_ids < live_size) & (col_ids <= row_ids)
    live_factor = jnp.where(keeping, factor, (row_ids == col_ids).astype(jnp.float32))
    panel_rows = lax.broadcasted_iota(jnp.int32, gluing.shape, 0)
    live_panel = jnp.where(panel_rows < live_size, gluing, jnp.zeros_like(gluing))
    solved = lax.linalg.triangular_solve(live_factor, live_panel, left_side=True, lower=True)
    return lax.dot_general(solved.astype(jnp.float32), solved.astype(jnp.float32), (((0,), (0,)), ((), ())), precision=lax.Precision.HIGHEST, preferred_element_type=jnp.float32)

def reference(factors, panels, sizes, glue_index, loads):
    local_dual = lax.map(one_subdomain, (factors, panels, sizes))
    per_cluster = SUB_DEV * N_MEMBER
    cluster_of = (jnp.arange(SUBS, dtype=jnp.int32) // per_cluster).astype(jnp.int32)
    assembled = jnp.zeros((N_CLUSTER, NDUAL, NDUAL), jnp.float32)
    assembled = assembled.at[cluster_of[:, None, None], glue_index[:, :, None], glue_index[:, None, :]].add(local_dual)
    dual_rows = assembled.reshape(N_CLUSTER * NDUAL, NDUAL)
    raw = jnp.einsum('cij,cjr->cir', assembled, loads.reshape(N_CLUSTER, NDUAL, NRHS), precision=lax.Precision.HIGHEST)
    row_share = NDUAL // N_MEMBER
    blocked = raw.reshape(N_CLUSTER, N_MEMBER, row_share, NRHS)
    previous_rows = jnp.roll(blocked, 1, axis=0)[:, :, row_share - IFACE:, :]
    next_rows = jnp.roll(blocked, -1, axis=0)[:, :, :IFACE, :]
    between = jnp.zeros((N_CLUSTER, N_MEMBER, row_share - 2 * IFACE, NRHS), jnp.float32)
    products = blocked + jnp.concatenate([previous_rows, between, next_rows], axis=2)
    return (dual_rows, products.reshape(N_CLUSTER * NDUAL, NRHS))
```

```python
import functools

import jax
import jax.numpy as jnp
from jax import lax
from jax.experimental import pallas as pl
from jax.experimental.pallas import tpu as pltpu
from jax.sharding import PartitionSpec as P

ORDER = 1024
PANEL = 256
NDUAL = 1024
MEMBERS = 32
CLUSTERS = 8
SHARE = NDUAL // MEMBERS
CAP = 2 * PANEL // MEMBERS
SUBS = 2
IFACE = 8
LANES = 128
STEP = 128
STEPS = ORDER // STEP
BASE = 32
TILES = NDUAL // LANES
F32, BF16, I32 = jnp.float32, jnp.bfloat16, jnp.int32
MESH = pl.DeviceIdType.MESH


def iota(shape, dim):
    return lax.broadcasted_iota(I32, shape, dim)


def split(x):
    high = x.astype(BF16)
    return high, (x - high.astype(F32)).astype(BF16)


def dot(a, b, dims=((1,), (0,))):
    return lax.dot_general(a, b, (dims, ((), ())), preferred_element_type=F32)


def dot3(a, b):
    a_high, a_low = a
    b_high, b_low = b
    left = jnp.concatenate([a_high, a_low], axis=1)
    right = jnp.concatenate([b_high, b_high], axis=0)
    return dot(left, right) + dot(a_high, b_low)


def lanes_from(x, index):
    return jnp.take_along_axis(x, index, axis=1, mode="promise_in_bounds")


def base_inverses(block):
    group = iota((BASE, LANES), 1) // BASE
    packed = jnp.zeros((BASE, LANES), F32)
    for q in range(LANES // BASE):
        packed = jnp.where(group == q, block[q * BASE : (q + 1) * BASE], packed)
    count = BASE // 8
    lane = iota((8, LANES), 1)
    first = (lane // BASE) * BASE
    unit, within, start, scale = [], lane % BASE, [], jnp.zeros((1, LANES), F32)
    for v in range(count):
        rows = packed[v * 8 : (v + 1) * 8]
        row_id = iota((8, LANES), 0) + v * 8
        inverse = 1.0 / lanes_from(rows, first + row_id)
        unit.append(jnp.where(within < row_id, rows * inverse, 0.0))
        start.append(jnp.where(within == row_id, 1.0, 0.0))
        scale = scale + jnp.sum(jnp.where(within == row_id, inverse, 0.0), axis=0, keepdims=True)
    result = start
    for j in range(BASE - 1):
        row = jnp.broadcast_to(result[j // 8][j % 8 : j % 8 + 1], (8, LANES))
        for v in range((j + 1) // 8, count):
            result[v] = result[v] - lanes_from(unit[v], first + j) * row
    scaled = jnp.concatenate(result, axis=0) * scale
    return jnp.concatenate(
        [jnp.where(group == q, scaled, 0.0) for q in range(LANES // BASE)], axis=0
    )


def block_inverse(block):
    inverse = base_inverses(block)
    size = BASE
    while size < STEP:
        row, col = iota(block.shape, 0) // size, iota(block.shape, 1) // size
        below = split(jnp.where((row % 2 == 1) & (col == row - 1), block, 0.0))
        picked = [
            inverse[k * size : (k + 1) * size] for k in range(1, STEP // size, 2)
        ]
        lower = jnp.concatenate(picked, axis=0)
        change = dot3(split(dot3(split(lower), below)), split(inverse))
        pieces = []
        for k in range(STEP // size):
            piece = inverse[k * size : (k + 1) * size]
            if k % 2:
                piece = piece - change[(k // 2) * size : (k // 2 + 1) * size]
            pieces.append(piece)
        inverse = jnp.concatenate(pieces, axis=0)
        size *= 2
    return inverse


def kernel(
    sizes, factors, panels, glue, loads, dual_out, products_out,
    factor, rhs, solved_high, solved_low, diag_high, diag_low, dispatch,
    outgoing, incoming, columns, rank_rows, ranks, all_loads,
    spread_high, spread_low, placing, stacked, raw, before, after,
    factor_sem, panel_sem, value_send, value_recv, column_send, column_recv,
    rank_send, rank_recv, load_send, load_recv, end_send, end_recv,
):
    me = lax.axis_index("member")
    cluster = lax.axis_index("cluster")
    following = lax.rem(cluster + 1, CLUSTERS)
    preceding = lax.rem(cluster + CLUSTERS - 1, CLUSTERS)

    def panel_copy(s):
        return pltpu.make_async_copy(panels.at[s], rhs.at[s], panel_sem.at[s])

    def factor_copy(s, i):
        rows, cols = pl.ds(i * STEP, STEP), pl.ds(0, (i + 1) * STEP)
        return pltpu.make_async_copy(
            factors.at[s, rows, cols], factor.at[s, rows, cols], factor_sem.at[s, i]
        )

    for s in range(SUBS):
        for i in range(STEPS):
            factor_copy(s, i).start()
        panel_copy(s).start()

    barrier = pltpu.get_barrier_semaphore()

    @pl.loop(1, MEMBERS)
    def _(o):
        to = lax.rem(me + o, MEMBERS)
        pl.semaphore_signal(barrier, inc=1, device_id=(cluster, to), device_id_type=MESH)

    for other in (following, preceding):
        pl.semaphore_signal(barrier, inc=1, device_id=(other, me), device_id_type=MESH)

    row16, col16 = iota((16, PANEL), 0), iota((16, PANEL), 1)
    probe = jnp.where(row16 == 0, 1, jnp.where(row16 == 1, col16, 0)).astype(F32).astype(BF16)
    up_row, up_col = iota((LANES, LANES), 0), iota((LANES, LANES), 1)
    earlier = jnp.where((up_row // SHARE == up_col // SHARE) & (up_row < up_col), 1.0, 0.0)
    earlier = earlier.astype(BF16)
    for s in range(SUBS):
        glued = glue[s : s + 1, :]
        hot = jnp.where(iota((NDUAL, PANEL), 0) == glued, 1.0, 0.0).astype(BF16)
        found = dot(probe, hot, ((1,), (1,)))
        tiles = jnp.concatenate(
            [found[:, t * LANES : (t + 1) * LANES] for t in range(TILES)], axis=0
        )
        counts = dot(tiles.astype(BF16), earlier)
        for t in range(TILES):
            there = tiles[16 * t : 16 * t + 1] > 0.5
            where_from = tiles[16 * t + 1 : 16 * t + 2].astype(I32)
            columns[me * SUBS + s, t : t + 1, :] = jnp.where(there, where_from, PANEL)
            rank_rows[t, s : s + 1, :] = jnp.where(
                there, counts[16 * t : 16 * t + 1].astype(I32), -1
            )
        wide = jnp.concatenate([counts[16 * t : 16 * t + 16] for t in range(TILES)], axis=1)
        rank = dot(wide.astype(BF16), hot)[0:1].astype(I32)
        target = (glued // SHARE) * CAP + rank
        picks = jnp.where(iota((MEMBERS * CAP, PANEL), 0) == target, 1.0, 0.0)
        dispatch[s] = picks.astype(BF16)

    pl.semaphore_wait(barrier, MEMBERS + 1)

    def to_member(src, dst, send, recv, to):
        return pltpu.make_async_remote_copy(
            src_ref=src, dst_ref=dst, send_sem=send, recv_sem=recv,
            device_id=(cluster, to), device_id_type=MESH,
        )

    mine = pl.ds(me * SUBS, SUBS)

    @pl.loop(1, MEMBERS)
    def _(o):
        to = lax.rem(me + o, MEMBERS)
        to_member(columns.at[mine], columns.at[mine], column_send, column_recv.at[me], to).start()
        to_member(
            rank_rows.at[to // (LANES // SHARE)], ranks.at[me], rank_send, rank_recv.at[me], to
        ).start()
        to_member(loads, all_loads.at[me], load_send, load_recv.at[me], to).start()

    def solve(s):
        live = sizes[s]
        for i in range(STEPS):
            factor_copy(s, i).wait()
        for i in range(STEPS):
            rows = pl.ds(i * STEP, STEP)
            square = factor[s, rows, rows]
            row_id = iota(square.shape, 0)
            col_id = iota(square.shape, 1)
            keep = (col_id <= row_id) & (row_id + i * STEP < live)
            square = jnp.where(keep, square, jnp.where(row_id == col_id, 1.0, 0.0))
            high, low = split(block_inverse(square))
            diag_high[i] = high
            diag_low[i] = low
        panel_copy(s).wait()
        for i in range(STEPS):
            rows = pl.ds(i * STEP, STEP)
            part = rhs[s, rows, :]
            part = jnp.where(iota(part.shape, 0) + i * STEP < live, part, 0.0)
            found = split(dot3((diag_high[i], diag_low[i]), split(part)))
            solved_high[rows, :], solved_low[rows, :] = found
            if i < STEPS - 1:
                rest = pl.ds((i + 1) * STEP, ORDER - (i + 1) * STEP)
                rhs[s, rest, :] = rhs[s, rest, :] - dot3(split(factor[s, rest, rows]), found)
        high = solved_high[...]
        cross = dot(high, solved_low[...], ((0,), (0,)))
        local = dot(high, high, ((0,), (0,))) + (cross + cross.T)
        local_high, local_low = split(local)
        picks = dispatch[s]
        values = dot(picks, local_high) + dot(picks, local_low)
        outgoing[s] = values.reshape(MEMBERS, CAP, PANEL)
        incoming[s, me] = outgoing[s, me]

    @pl.loop(0, SUBS)
    def _(s):
        solve(s)

        @pl.loop(1, MEMBERS)
        def _(o):
            to = lax.rem(me + o, MEMBERS)
            to_member(
                outgoing.at[s, to], incoming.at[s, me], value_send.at[s], value_recv.at[s, me], to
            ).start()

    all_loads[me] = loads[...]
    ranks[me] = rank_rows[me // (LANES // SHARE)]

    @pl.loop(1, MEMBERS)
    def _(o):
        source = lax.rem(me - o + MEMBERS, MEMBERS)
        theirs = pl.ds(source * SUBS, SUBS)
        to_member(columns.at[theirs], columns.at[theirs], column_send, column_recv.at[source], source).wait_recv()
        to_member(rank_rows.at[0], ranks.at[source], rank_send, rank_recv.at[source], source).wait_recv()
        to_member(loads, all_loads.at[source], load_send, load_recv.at[source], source).wait_recv()

    slot = iota((CAP, LANES), 0)
    for s in range(SUBS):

        @pl.loop(0, MEMBERS)
        def _(o):
            source = lax.rem(me - o + MEMBERS, MEMBERS)

            @pl.when(o > 0)
            def _():
                to_member(
                    outgoing.at[s, 0], incoming.at[s, source], value_send.at[s],
                    value_recv.at[s, source], source,
                ).wait_recv()

            rows = pl.ds(pl.multiple_of((s * MEMBERS + o) * CAP, CAP), CAP)
            left = incoming[s, source, :, 0:LANES]
            right = incoming[s, source, :, LANES : 2 * LANES]
            for t in range(TILES):
                index = jnp.broadcast_to(columns[source * SUBS + s, t : t + 1, :], (CAP, LANES))
                lane = index & (LANES - 1)
                value = jnp.where(index < LANES, lanes_from(left, lane), lanes_from(right, lane))
                value = jnp.where(index < PANEL, value, 0.0)
                high, low = split(value)
                spread_high[rows, t * LANES : (t + 1) * LANES] = high
                spread_low[rows, t * LANES : (t + 1) * LANES] = low
            here = jnp.where(slot == ranks[source, s : s + 1, :], 1.0, 0.0)
            placing[rows, :] = here.astype(BF16)

    place = placing[...]
    stacked[...] = dot(place, spread_high[...], ((0,), (0,))) + dot(
        place, spread_low[...], ((0,), (0,))
    )
    owned = stacked[pl.ds(pl.multiple_of(lax.rem(me, LANES // SHARE) * SHARE, SHARE), SHARE), :]
    all_high, all_low = split(all_loads[...].reshape(NDUAL, PANEL))
    owned_high, owned_low = split(owned)
    product = dot(owned_high, all_high) + dot(owned_low, all_high) + dot(owned_high, all_low)
    raw[...] = product
    dual_out[...] = owned

    def end_copy(src, dst, k, to):
        return pltpu.make_async_remote_copy(
            src_ref=src, dst_ref=dst, send_sem=end_send.at[k], recv_sem=end_recv.at[k],
            device_id=(to, me), device_id_type=MESH,
        )

    up = end_copy(raw.at[pl.ds(SHARE - IFACE, IFACE)], before, 0, following)
    down = end_copy(raw.at[pl.ds(0, IFACE)], after, 1, preceding)
    up.start()
    down.start()
    products_out[pl.ds(IFACE, SHARE - 2 * IFACE), :] = product[IFACE : SHARE - IFACE]
    up.wait()
    down.wait()
    products_out[pl.ds(0, IFACE), :] = product[0:IFACE] + before[...]
    products_out[pl.ds(SHARE - IFACE, IFACE), :] = product[SHARE - IFACE :] + after[...]

    others = pl.ds(0, MEMBERS - 1)
    for s in range(SUBS):
        pltpu.make_async_copy(outgoing.at[s, others], incoming.at[s, others], value_send.at[s]).wait()
    pltpu.make_async_copy(
        columns.at[pl.ds(0, SUBS * (MEMBERS - 1))], columns.at[pl.ds(0, SUBS * (MEMBERS - 1))], column_send
    ).wait()
    pltpu.make_async_copy(ranks.at[others], ranks.at[others], rank_send).wait()
    pltpu.make_async_copy(all_loads.at[others], all_loads.at[others], load_send).wait()


def on_device(factors, panels, sizes, glue_index, loads):
    vmem = pl.BlockSpec(memory_space=pltpu.VMEM)
    dma = pltpu.SemaphoreType.DMA
    return pl.pallas_call(
        kernel,
        out_shape=(
            jax.ShapeDtypeStruct((SHARE, NDUAL), F32),
            jax.ShapeDtypeStruct((SHARE, PANEL), F32),
        ),
        in_specs=[
            pl.BlockSpec(memory_space=pltpu.SMEM),
            pl.BlockSpec(memory_space=pl.ANY),
            pl.BlockSpec(memory_space=pl.ANY),
            vmem,
            vmem,
        ],
        out_specs=(vmem, vmem),
        scratch_shapes=[
            pltpu.VMEM((SUBS, ORDER, ORDER), F32),
            pltpu.VMEM((SUBS, ORDER, PANEL), F32),
            pltpu.VMEM((ORDER, PANEL), BF16),
            pltpu.VMEM((ORDER, PANEL), BF16),
            pltpu.VMEM((STEPS, STEP, STEP), BF16),
            pltpu.VMEM((STEPS, STEP, STEP), BF16),
            pltpu.VMEM((SUBS, MEMBERS * CAP, PANEL), BF16),
            pltpu.VMEM((SUBS, MEMBERS, CAP, PANEL), F32),
            pltpu.VMEM((SUBS, MEMBERS, CAP, PANEL), F32),
            pltpu.VMEM((MEMBERS * SUBS, TILES, LANES), I32),
            pltpu.VMEM((TILES, SUBS, LANES), I32),
            pltpu.VMEM((MEMBERS, SUBS, LANES), I32),
            pltpu.VMEM((MEMBERS, SHARE, PANEL), F32),
            pltpu.VMEM((SUBS * MEMBERS * CAP, NDUAL), BF16),
            pltpu.VMEM((SUBS * MEMBERS * CAP, NDUAL), BF16),
            pltpu.VMEM((SUBS * MEMBERS * CAP, LANES), BF16),
            pltpu.VMEM((LANES, NDUAL), F32),
            pltpu.VMEM((SHARE, PANEL), F32),
            pltpu.VMEM((IFACE, PANEL), F32),
            pltpu.VMEM((IFACE, PANEL), F32),
            dma((SUBS, STEPS)),
            dma((SUBS,)),
            dma((SUBS,)),
            dma((SUBS, MEMBERS)),
            dma,
            dma((MEMBERS,)),
            dma,
            dma((MEMBERS,)),
            dma,
            dma((MEMBERS,)),
            dma((2,)),
            dma((2,)),
        ],
        compiler_params=pltpu.CompilerParams(
            collective_id=0, has_side_effects=True, vmem_limit_bytes=56 * 2**20
        ),
        name="dual_operator",
    )(sizes, factors, panels, glue_index, loads)


def solution(mesh):
    whole = ("cluster", "member")
    return jax.shard_map(
        on_device,
        mesh=mesh,
        in_specs=(P(whole, None, None), P(whole, None, None), P(whole), P(whole, None), P(whole, None)),
        out_specs=(P(whole, None), P(whole, None)),
        check_vma=False,
    )
```

```python
import functools

import jax
import jax.numpy as jnp
from jax import lax
from jax.experimental import pallas as pl
from jax.experimental.pallas import tpu as pltpu
from jax.sharding import PartitionSpec as P

ORDER = 1024
PANEL = 256
NDUAL = 1024
MEMBERS = 32
CLUSTERS = 8
CORES = 2
CHIPS = MEMBERS // CORES
SIDE = 4
AROUND = [(dx, dy) for dy in (1, 3, 2, 0) for dx in (1, 3, 0, 2) if (dx, dy) != (0, 0)]
GROUP = 8
SHARE = NDUAL // MEMBERS
CAP = 2 * PANEL // MEMBERS
SUBS = 2
IFACE = 8
LANES = 128
STEP = 128
STEPS = ORDER // STEP
BATCH = 4
FOLD = 4
BASE = 32
TILES = NDUAL // LANES
F32, BF16, I32 = jnp.float32, jnp.bfloat16, jnp.int32
MESH = pl.DeviceIdType.MESH


def iota(shape, dim):
    return lax.broadcasted_iota(I32, shape, dim)


def split(x):
    high = x.astype(BF16)
    return high, (x - high.astype(F32)).astype(BF16)


def dot(a, b, dims=((1,), (0,))):
    return lax.dot_general(a, b, (dims, ((), ())), preferred_element_type=F32)


def dot3(a, b):
    a_high, a_low = a
    b_high, b_low = b
    left = jnp.concatenate([a_high, a_low], axis=1)
    right = jnp.concatenate([b_high, b_high], axis=0)
    return dot(left, right) + dot(a_high, b_low)


def lanes_from(x, index):
    numbers = lax.GatherDimensionNumbers(
        offset_dims=(),
        collapsed_slice_dims=(1,),
        start_index_map=(1,),
        operand_batching_dims=(0,),
        start_indices_batching_dims=(0,),
    )
    return lax.gather(
        x, index[..., None], numbers, (1, 1), mode=lax.GatherScatterMode.PROMISE_IN_BOUNDS
    )


def base_inverses(blocks):
    count = BASE // 8
    group = iota((BASE, LANES), 1) // BASE
    lane = iota((8, LANES), 1)
    first, within = (lane // BASE) * BASE, lane % BASE
    row_ids = [iota((8, LANES), 0) + v * 8 for v in range(count)]
    units, results, scales = [], [], []
    for block in blocks:
        packed = jnp.zeros((BASE, LANES), F32)
        for q in range(LANES // BASE):
            packed = jnp.where(group == q, block[q * BASE : (q + 1) * BASE], packed)
        unit, scale = [], jnp.zeros((1, LANES), F32)
        for v in range(count):
            rows = packed[v * 8 : (v + 1) * 8]
            inverse = 1.0 / lanes_from(rows, first + row_ids[v])
            unit.append(jnp.where(within < row_ids[v], rows * inverse, 0.0))
            own = jnp.where(within == row_ids[v], inverse, 0.0)
            scale = scale + jnp.sum(own, axis=0, keepdims=True)
        units.append(unit)
        scales.append(scale)
        results.append([jnp.where(within == row_ids[v], 1.0, 0.0) for v in range(count)])
    for j in range(BASE - 1):
        for unit, result in zip(units, results):
            row = jnp.broadcast_to(result[j // 8][j % 8 : j % 8 + 1], (8, LANES))
            for v in range((j + 1) // 8, count):
                result[v] = result[v] - lanes_from(unit[v], first + j) * row
    inverses = []
    for result, scale in zip(results, scales):
        scaled = jnp.concatenate(result, axis=0) * scale
        inverses.append(
            jnp.concatenate(
                [jnp.where(group == q, scaled, 0.0) for q in range(LANES // BASE)], axis=0
            )
        )
    return inverses


def doubled(inverses, blocks, size):
    row, col = iota((STEP, STEP), 0) // size, iota((STEP, STEP), 1) // size
    below = (row % 2 == 1) & (col == row - 1)
    odd = range(1, STEP // size, 2)
    halves = [split(inverse) for inverse in inverses]
    firsts = []
    for (high, low), block in zip(halves, blocks):
        lower = [
            jnp.concatenate([part[k * size : (k + 1) * size] for k in odd], axis=0)
            for part in (high, low)
        ]
        firsts.append(dot3(lower, split(jnp.where(below, block, 0.0))))
    results = []
    for inverse, half, part in zip(inverses, halves, firsts):
        change = dot3(split(part), half)
        pieces = []
        for k in range(STEP // size):
            piece = inverse[k * size : (k + 1) * size]
            if k % 2:
                piece = piece - change[(k // 2) * size : (k // 2 + 1) * size]
            pieces.append(piece)
        results.append(jnp.concatenate(pieces, axis=0))
    return results


def kernel(
    sizes, factors, panels, glue, loads, dual_out, products_out,
    factor, rhs, solved_high, solved_low, step_high, step_low, dispatch,
    outgoing, incoming, columns, own_tile, ranks, all_loads, inverted,
    spread_high, spread_low, placing, stacked, raw, before, after,
    factor_sem, panel_sem, value_send, value_recv, column_send, column_recv,
    load_send, load_recv, pair_send, pair_recv, end_send, end_recv,
):
    me = lax.axis_index("member")
    cluster = lax.axis_index("cluster")
    chip, core = me // CORES, lax.rem(me, CORES)
    partner = chip * CORES + (1 - core)
    following = lax.rem(cluster + 1, CLUSTERS)
    preceding = lax.rem(cluster + CLUSTERS - 1, CLUSTERS)

    def panel_copy(s):
        return pltpu.make_async_copy(panels.at[s], rhs.at[s], panel_sem.at[s])

    def factor_copy(s, i):
        rows, cols = pl.ds(i * STEP, STEP), pl.ds(0, (i + 1) * STEP)
        return pltpu.make_async_copy(
            factors.at[s, rows, cols], factor.at[s, rows, cols], factor_sem.at[s, i]
        )

    for s in range(SUBS):
        for i in range(STEPS):
            factor_copy(s, i).start()
        panel_copy(s).start()

    barrier = pltpu.get_barrier_semaphore()

    @pl.loop(1, MEMBERS)
    def _(o):
        to = lax.rem(me + o, MEMBERS)
        pl.semaphore_signal(barrier, inc=1, device_id=(cluster, to), device_id_type=MESH)

    for other in (following, preceding):
        pl.semaphore_signal(barrier, inc=1, device_id=(other, me), device_id_type=MESH)

    row16, col16 = iota((16, PANEL), 0), iota((16, PANEL), 1)
    probe = jnp.where(row16 == 0, 1, jnp.where(row16 == 1, col16, 0)).astype(F32).astype(BF16)
    up_row, up_col = iota((LANES, LANES), 0), iota((LANES, LANES), 1)
    earlier = jnp.where((up_row // SHARE == up_col // SHARE) & (up_row < up_col), 1.0, 0.0)
    earlier = earlier.astype(BF16)
    for s in range(SUBS):
        glued = glue[s : s + 1, :]
        hot = jnp.where(iota((NDUAL, PANEL), 0) == glued, 1.0, 0.0).astype(BF16)
        found = dot(probe, hot, ((1,), (1,)))
        tiles = jnp.concatenate(
            [found[:, t * LANES : (t + 1) * LANES] for t in range(TILES)], axis=0
        )
        counts = dot(tiles.astype(BF16), earlier)
        for t in range(TILES):
            there = tiles[16 * t : 16 * t + 1] > 0.5
            where_from = tiles[16 * t + 1 : 16 * t + 2].astype(I32)
            columns[chip, core, s, t : t + 1, :] = jnp.where(there, where_from, PANEL)
        wide = jnp.concatenate([counts[16 * t : 16 * t + 16] for t in range(TILES)], axis=1)
        rank = dot(wide.astype(BF16), hot)[0:1].astype(I32)
        target = (glued // SHARE) * CAP + rank
        picks = jnp.where(iota((MEMBERS * CAP, PANEL), 0) == target, 1.0, 0.0)
        dispatch[s] = picks.astype(BF16)

    def to_member(src, dst, send, recv, to):
        return pltpu.make_async_remote_copy(
            src_ref=src, dst_ref=dst, send_sem=send, recv_sem=recv,
            device_id=(cluster, to), device_id_type=MESH,
        )

    def chip_at(dx, dy):
        y, x = chip // SIDE, lax.rem(chip, SIDE)
        return lax.rem(y + dy, SIDE) * SIDE + lax.rem(x + dx, SIDE)

    def squares(s):
        live = sizes[s]
        found = []
        for i in range(STEPS):
            rows = pl.ds(i * STEP, STEP)
            square = factor[s, rows, rows]
            row_id, col_id = iota(square.shape, 0), iota(square.shape, 1)
            keep = (col_id <= row_id) & (row_id + i * STEP < live)
            found.append(jnp.where(keep, square, jnp.where(row_id == col_id, 1.0, 0.0)))
        return found

    def invert(s):
        for i in range(STEPS):
            factor_copy(s, i).wait()
        blocks = squares(s)
        for k in range(0, STEPS, BATCH):
            for i, found in enumerate(base_inverses(blocks[k : k + BATCH])):
                inverted[k + i] = found
        found = [inverted[i] for i in range(STEPS)]
        size = BASE
        while size < STEP:
            found = doubled(found, blocks, size)
            size *= 2
        for i in range(STEPS):
            half = split(found[i])
            step_high[s, i, 0:STEP], step_low[s, i, 0:STEP] = half
            if i < STEPS - 1:
                under = factor[s, pl.ds((i + 1) * STEP, STEP), pl.ds(i * STEP, STEP)]
                onward = split(dot3(split(under), half))
                step_high[s, i, STEP : 2 * STEP], step_low[s, i, STEP : 2 * STEP] = onward

    with jax.named_scope("invert"):
        invert(0)

    with jax.named_scope("barrier"):
        pl.semaphore_wait(barrier, MEMBERS + 1)

    def chip_at(dx, dy):
        y, x = chip // SIDE, lax.rem(chip, SIDE)
        return lax.rem(y + dy, SIDE) * SIDE + lax.rem(x + dx, SIDE)

    def along(first, second):
        return chip_at(
            first * (1 - core) + second * core, first * core + second * (1 - core)
        )

    def column_copy(origin, to):
        return to_member(
            columns.at[origin, core], columns.at[origin, core], column_send,
            column_recv.at[origin], to * CORES + core,
        )

    def load_copy(source, origin, to):
        return to_member(
            source, all_loads.at[origin, core], load_send, load_recv.at[origin], to * CORES + core
        )

    every = pl.ds(0, CHIPS)

    def pair_copy(ref, which, k):
        return to_member(
            ref.at[every, which], ref.at[every, which], pair_send.at[k], pair_recv.at[k], partner
        )

    with jax.named_scope("share"):
        for dx, dy in AROUND:
            column_copy(chip, chip_at(dx, dy)).start()
        for k in (1, 3, 2):
            load_copy(loads, chip, along(k, 0)).start()
            load_copy(loads, chip, along(0, k)).start()
        all_loads[chip, core] = loads[...]

    def substitute(s):
        live = sizes[s]
        panel_copy(s).wait()

        def masked(i, part):
            return jnp.where(iota(part.shape, 0) + i * STEP < live, part, 0.0)

        part = masked(0, rhs[s, 0:STEP, :])
        squared, cross = [], []
        for i in range(STEPS):
            halves = split(part)
            tall = STEP if i == STEPS - 1 else 2 * STEP
            both = dot3((step_high[s, i, 0:tall], step_low[s, i, 0:tall]), halves)
            if i < STEPS - 1:
                part = masked(i + 1, rhs[s, (i + 1) * STEP : (i + 2) * STEP, :] - both[STEP:])
            found = split(both[0:STEP])
            solved_high[i * STEP : (i + 1) * STEP], solved_low[i * STEP : (i + 1) * STEP] = found
            if i < STEPS - 2:
                rest = pl.ds((i + 2) * STEP, ORDER - (i + 2) * STEP)
                left = split(factor[s, rest, pl.ds(i * STEP, STEP)])
                rhs[s, rest, :] = rhs[s, rest, :] - dot3(left, found)
            if i % FOLD == FOLD - 1:
                done = pl.ds((i + 1 - FOLD) * STEP, FOLD * STEP)
                high = solved_high[done, :]
                squared.append(dot(high, high, ((0,), (0,))))
                cross.append(dot(high, solved_low[done, :], ((0,), (0,))))
        crossed = sum(cross[1:], cross[0])
        local = sum(squared[1:], squared[0]) + (crossed + crossed.T)
        local_high, local_low = split(local)
        picks = dispatch[s]
        values = dot(picks, local_high) + dot(picks, local_low)
        outgoing[s] = values.reshape(MEMBERS, CAP, PANEL)
        incoming[s, me] = outgoing[s, me]

    for s in range(SUBS):
        if s:
            with jax.named_scope("invert"):
                invert(1)

            with jax.named_scope("forward"):
                for first in (3, 1, 2):
                    origin = along(first, 0)
                    load_copy(loads, origin, origin).wait_recv()
                    for k in (1, 3, 2):
                        load_copy(all_loads.at[origin, core], origin, along(0, k)).start()
                for dx, dy in AROUND:
                    origin = chip_at(dx, dy)
                    column_copy(origin, origin).wait_recv()
                pair_copy(columns, core, 0).start()

        with jax.named_scope("substitute"):
            substitute(s)

        def send(to):
            to_member(
                outgoing.at[s, to], incoming.at[s, me], value_send.at[s], value_recv.at[s, me], to
            ).start()

        with jax.named_scope("send"):

            @pl.loop(0, CORES)
            def _(dc):
                for dx, dy in AROUND:
                    send(chip_at(dx, dy) * CORES + lax.rem(core + dc, CORES))

            send(partner)

    with jax.named_scope("pair"):
        pair_copy(columns, 1 - core, 0).wait_recv()

    with jax.named_scope("ranks"):
        @pl.loop(0, MEMBERS)
        def _(m):
            for s in range(SUBS):
                tile = columns[m // CORES, lax.rem(m, CORES), s, pl.ds(me // (LANES // SHARE), 1), :]
                own_tile[pl.ds(s * MEMBERS + m, 1), :] = tile

        shift = lax.rem(me, LANES // SHARE) * SHARE
        own = own_tile[...]
        lane = iota(own.shape, 1)
        own = lanes_from(own, lax.rem(lane + shift, LANES))
        there = (own < PANEL) & (lane < SHARE)
        order = dot(jnp.where(there, 1.0, 0.0).astype(BF16), earlier).astype(I32)
        ranks[...] = jnp.where(there, order, -1)

    slot = iota((CAP, LANES), 0)
    stacked[...] = jnp.zeros_like(stacked)

    def place_one(s, source, k):
        rows = slice(k * CAP, (k + 1) * CAP)
        left = incoming[s, source, :, 0:LANES]
        right = incoming[s, source, :, LANES : 2 * LANES]
        source_chip, source_core = source // CORES, lax.rem(source, CORES)
        for t in range(TILES):
            index = jnp.broadcast_to(columns[source_chip, source_core, s, t : t + 1, :], (CAP, LANES))
            lane = index & (LANES - 1)
            value = jnp.where(index < LANES, lanes_from(left, lane), lanes_from(right, lane))
            value = jnp.where(index < PANEL, value, 0.0)
            high, low = split(value)
            spread_high[rows, t * LANES : (t + 1) * LANES] = high
            spread_low[rows, t * LANES : (t + 1) * LANES] = low
        here = jnp.where(slot == ranks[pl.ds(s * MEMBERS + source, 1), :], 1.0, 0.0)
        placing[rows, :] = here.astype(BF16)

    for s in range(SUBS):
        with jax.named_scope("place"):

            @pl.loop(0, CORES)
            def _(dc):
                if s:

                    @pl.when(dc == CORES - 1)
                    def _():
                        for second in (1, 3, 2):
                            for first in range(SIDE):
                                origin = along(first, second)
                                load_copy(loads, origin, origin).wait_recv()
                        pair_copy(all_loads, core, 1).start()

                for half in range(CHIPS // GROUP):
                    sources = [
                        chip_at((SIDE - dx) % SIDE, (SIDE - dy) % SIDE) * CORES
                        + lax.rem(core + dc, CORES)
                        for dx, dy in (AROUND + [(0, 0)])[half * GROUP : (half + 1) * GROUP]
                    ]

                    def wait(source):
                        to_member(
                            outgoing.at[s, 0], incoming.at[s, source], value_send.at[s],
                            value_recv.at[s, source], source,
                        ).wait_recv()

                    last = half == CHIPS // GROUP - 1
                    for source in sources[:-1] if last else sources:
                        wait(source)
                    if last:
                        pl.when(dc > 0)(functools.partial(wait, partner))
                    for k, source in enumerate(sources):
                        place_one(s, source, k)
                    place = placing[...]
                    part = dot(place, spread_high[...], ((0,), (0,))) + dot(
                        place, spread_low[...], ((0,), (0,))
                    )
                    part = part[0:SHARE]
                    stacked[...] = stacked[...] + part

    with jax.named_scope("apply"):
        pair_copy(all_loads, 1 - core, 1).wait_recv()
        owned = stacked[...]
        all_high, all_low = split(all_loads[...].reshape(NDUAL, PANEL))
        owned_high, owned_low = split(owned)
        product = dot(owned_high, all_high) + dot(owned_low, all_high) + dot(owned_high, all_low)
        raw[...] = product
        dual_out[...] = owned

    def end_copy(src, dst, k, to):
        return pltpu.make_async_remote_copy(
            src_ref=src, dst_ref=dst, send_sem=end_send.at[k], recv_sem=end_recv.at[k],
            device_id=(to, me), device_id_type=MESH,
        )

    up = end_copy(raw.at[pl.ds(SHARE - IFACE, IFACE)], before, 0, following)
    down = end_copy(raw.at[pl.ds(0, IFACE)], after, 1, preceding)
    with jax.named_scope("ends"):
        up.start()
        down.start()
        products_out[pl.ds(IFACE, SHARE - 2 * IFACE), :] = product[IFACE : SHARE - IFACE]
        up.wait()
        down.wait()
        products_out[pl.ds(0, IFACE), :] = product[0:IFACE] + before[...]
        products_out[pl.ds(SHARE - IFACE, IFACE), :] = product[SHARE - IFACE :] + after[...]

    others = pl.ds(0, MEMBERS - 1)
    with jax.named_scope("drain"):
        for s in range(SUBS):
            pltpu.make_async_copy(outgoing.at[s, others], incoming.at[s, others], value_send.at[s]).wait()
        far = pl.ds(0, CHIPS - 1)
        pltpu.make_async_copy(columns.at[far, 0], columns.at[far, 0], column_send).wait()
        pltpu.make_async_copy(all_loads.at[far, 0], all_loads.at[far, 0], load_send).wait()
        pair_copy(columns, core, 0).wait_send()
        pair_copy(all_loads, core, 1).wait_send()


def hand_over(owned, products, owned_out, products_out):
    owned_out[...] = owned[...]
    products_out[...] = products[...]


def on_device(factors, panels, sizes, glue_index, loads):
    vmem = pl.BlockSpec(memory_space=pltpu.VMEM)
    dma = pltpu.SemaphoreType.DMA
    owned, products = pl.pallas_call(
        kernel,
        out_shape=(
            jax.ShapeDtypeStruct((SHARE, NDUAL), F32),
            jax.ShapeDtypeStruct((SHARE, PANEL), F32),
        ),
        in_specs=[
            pl.BlockSpec(memory_space=pltpu.SMEM),
            pl.BlockSpec(memory_space=pl.ANY),
            pl.BlockSpec(memory_space=pl.ANY),
            vmem,
            vmem,
        ],
        out_specs=(vmem, vmem),
        scratch_shapes=[
            pltpu.VMEM((SUBS, ORDER, ORDER), F32),
            pltpu.VMEM((SUBS, ORDER, PANEL), F32),
            pltpu.VMEM((ORDER, PANEL), BF16),
            pltpu.VMEM((ORDER, PANEL), BF16),
            pltpu.VMEM((SUBS, STEPS, 2 * STEP, STEP), BF16),
            pltpu.VMEM((SUBS, STEPS, 2 * STEP, STEP), BF16),
            pltpu.VMEM((SUBS, MEMBERS * CAP, PANEL), BF16),
            pltpu.VMEM((SUBS, MEMBERS, CAP, PANEL), F32),
            pltpu.VMEM((SUBS, MEMBERS, CAP, PANEL), F32),
            pltpu.VMEM((CHIPS, CORES, SUBS, TILES, LANES), I32),
            pltpu.VMEM((SUBS * MEMBERS, LANES), I32),
            pltpu.VMEM((SUBS * MEMBERS, LANES), I32),
            pltpu.VMEM((CHIPS, CORES, SHARE, PANEL), F32),
            pltpu.VMEM((STEPS, STEP, STEP), F32),
            pltpu.VMEM((GROUP * CAP, NDUAL), BF16),
            pltpu.VMEM((GROUP * CAP, NDUAL), BF16),
            pltpu.VMEM((GROUP * CAP, LANES), BF16),
            pltpu.VMEM((SHARE, NDUAL), F32),
            pltpu.VMEM((SHARE, PANEL), F32),
            pltpu.VMEM((IFACE, PANEL), F32),
            pltpu.VMEM((IFACE, PANEL), F32),
            dma((SUBS, STEPS)),
            dma((SUBS,)),
            dma((SUBS,)),
            dma((SUBS, MEMBERS)),
            dma,
            dma((CHIPS,)),
            dma,
            dma((CHIPS,)),
            dma((2,)),
            dma((2,)),
            dma((2,)),
            dma((2,)),
        ],
        compiler_params=pltpu.CompilerParams(
            collective_id=0, has_side_effects=True, vmem_limit_bytes=56 * 2**20
        ),
        name="dual_operator",
    )(sizes, factors, panels, glue_index, loads)
    return pl.pallas_call(
        hand_over,
        out_shape=(
            jax.ShapeDtypeStruct((SHARE, NDUAL), F32),
            jax.ShapeDtypeStruct((SHARE, PANEL), F32),
        ),
        in_specs=[vmem, vmem],
        out_specs=(vmem, vmem),
        name="hand_over",
    )(owned, products)


def solution(mesh):
    whole = ("cluster", "member")
    return jax.shard_map(
        on_device,
        mesh=mesh,
        in_specs=(P(whole, None, None), P(whole, None, None), P(whole), P(whole, None), P(whole, None)),
        out_specs=(P(whole, None), P(whole, None)),
        check_vma=False,
    )
```

```python
import functools

import jax
import jax.numpy as jnp
from jax import lax
from jax.experimental import pallas as pl
from jax.experimental.pallas import tpu as pltpu
from jax.sharding import PartitionSpec as P

ORDER = 1024
PANEL = 256
NDUAL = 1024
MEMBERS = 32
CLUSTERS = 8
CORES = 2
CHIPS = MEMBERS // CORES
SIDE = 4
AROUND = [(dx, dy) for dy in (1, 3, 2, 0) for dx in (1, 3, 0, 2) if (dx, dy) != (0, 0)]
GROUP = 4
SHARE = NDUAL // MEMBERS
CAP = 2 * PANEL // MEMBERS
SUBS = 2
IFACE = 8
LANES = 128
STEP = 128
STEPS = ORDER // STEP
BATCH = 4
FOLD = 4
BASE = 32
TILES = NDUAL // LANES
F32, BF16, I32 = jnp.float32, jnp.bfloat16, jnp.int32
MESH = pl.DeviceIdType.MESH


def iota(shape, dim):
    return lax.broadcasted_iota(I32, shape, dim)


def split(x):
    high = x.astype(BF16)
    return high, (x - high.astype(F32)).astype(BF16)


def dot(a, b, dims=((1,), (0,))):
    return lax.dot_general(a, b, (dims, ((), ())), preferred_element_type=F32)


def dot3(a, b):
    a_high, a_low = a
    b_high, b_low = b
    left = jnp.concatenate([a_high, a_low], axis=1)
    right = jnp.concatenate([b_high, b_high], axis=0)
    return dot(left, right) + dot(a_high, b_low)


def lanes_from(x, index):
    numbers = lax.GatherDimensionNumbers(
        offset_dims=(),
        collapsed_slice_dims=(1,),
        start_index_map=(1,),
        operand_batching_dims=(0,),
        start_indices_batching_dims=(0,),
    )
    return lax.gather(
        x, index[..., None], numbers, (1, 1), mode=lax.GatherScatterMode.PROMISE_IN_BOUNDS
    )


def base_inverses(blocks):
    count = BASE // 8
    group = iota((BASE, LANES), 1) // BASE
    lane = iota((8, LANES), 1)
    first, within = (lane // BASE) * BASE, lane % BASE
    row_ids = [iota((8, LANES), 0) + v * 8 for v in range(count)]
    units, results, scales = [], [], []
    for block in blocks:
        packed = jnp.zeros((BASE, LANES), F32)
        for q in range(LANES // BASE):
            packed = jnp.where(group == q, block[q * BASE : (q + 1) * BASE], packed)
        unit, scale = [], jnp.zeros((1, LANES), F32)
        for v in range(count):
            rows = packed[v * 8 : (v + 1) * 8]
            inverse = 1.0 / lanes_from(rows, first + row_ids[v])
            unit.append(jnp.where(within < row_ids[v], rows * inverse, 0.0))
            own = jnp.where(within == row_ids[v], inverse, 0.0)
            scale = scale + jnp.sum(own, axis=0, keepdims=True)
        units.append(unit)
        scales.append(scale)
        results.append([jnp.where(within == row_ids[v], 1.0, 0.0) for v in range(count)])
    for j in range(BASE - 1):
        for unit, result in zip(units, results):
            row = jnp.broadcast_to(result[j // 8][j % 8 : j % 8 + 1], (8, LANES))
            for v in range((j + 1) // 8, count):
                result[v] = result[v] - lanes_from(unit[v], first + j) * row
    inverses = []
    for result, scale in zip(results, scales):
        scaled = jnp.concatenate(result, axis=0) * scale
        inverses.append(
            jnp.concatenate(
                [jnp.where(group == q, scaled, 0.0) for q in range(LANES // BASE)], axis=0
            )
        )
    return inverses


def doubled(inverses, blocks, size):
    row, col = iota((STEP, STEP), 0) // size, iota((STEP, STEP), 1) // size
    below = (row % 2 == 1) & (col == row - 1)
    odd = range(1, STEP // size, 2)
    halves = [split(inverse) for inverse in inverses]
    firsts = []
    for (high, low), block in zip(halves, blocks):
        lower = [
            jnp.concatenate([part[k * size : (k + 1) * size] for k in odd], axis=0)
            for part in (high, low)
        ]
        firsts.append(dot3(lower, split(jnp.where(below, block, 0.0))))
    results = []
    for inverse, half, part in zip(inverses, halves, firsts):
        change = dot3(split(part), half)
        pieces = []
        for k in range(STEP // size):
            piece = inverse[k * size : (k + 1) * size]
            if k % 2:
                piece = piece - change[(k // 2) * size : (k // 2 + 1) * size]
            pieces.append(piece)
        results.append(jnp.concatenate(pieces, axis=0))
    return results


def kernel(
    sizes, factors, panels, glue, loads, dual_out, products_out,
    factor, rhs, solved_high, solved_low, step_high, step_low,
    outgoing, incoming, columns, own_tile, ranks, all_loads, inverted,
    spread_high, spread_low, placing, stacked, raw, before, after,
    factor_sem, panel_sem, value_send, value_recv, column_send, column_recv,
    load_send, load_recv, pair_send, pair_recv, end_send, end_recv,
):
    me = lax.axis_index("member")
    cluster = lax.axis_index("cluster")
    chip, core = me // CORES, lax.rem(me, CORES)
    partner = chip * CORES + (1 - core)
    following = lax.rem(cluster + 1, CLUSTERS)
    preceding = lax.rem(cluster + CLUSTERS - 1, CLUSTERS)

    def panel_copy(s):
        return pltpu.make_async_copy(panels.at[s], rhs.at[s], panel_sem.at[s])

    def factor_copy(s, i):
        rows, cols = pl.ds(i * STEP, STEP), pl.ds(0, (i + 1) * STEP)
        return pltpu.make_async_copy(
            factors.at[s, rows, cols], factor.at[s, rows, cols], factor_sem.at[s, i]
        )

    def start_copies(s):
        for i in range(STEPS):
            factor_copy(s, i).start()
        panel_copy(s).start()

    start_copies(0)

    barrier = pltpu.get_barrier_semaphore()

    @pl.loop(1, MEMBERS)
    def _(o):
        to = lax.rem(me + o, MEMBERS)
        pl.semaphore_signal(barrier, inc=1, device_id=(cluster, to), device_id_type=MESH)

    for other in (following, preceding):
        pl.semaphore_signal(barrier, inc=1, device_id=(other, me), device_id_type=MESH)

    row16, col16 = iota((16, PANEL), 0), iota((16, PANEL), 1)
    probe = jnp.where(row16 == 0, 1, jnp.where(row16 == 1, col16, 0)).astype(F32).astype(BF16)
    up_row, up_col = iota((LANES, LANES), 0), iota((LANES, LANES), 1)
    earlier = jnp.where((up_row // SHARE == up_col // SHARE) & (up_row < up_col), 1.0, 0.0)
    earlier = earlier.astype(BF16)
    targets = []
    for s in range(SUBS):
        glued = glue[s : s + 1, :]
        hot = jnp.where(iota((NDUAL, PANEL), 0) == glued, 1.0, 0.0).astype(BF16)
        found = dot(probe, hot, ((1,), (1,)))
        tiles = jnp.concatenate(
            [found[:, t * LANES : (t + 1) * LANES] for t in range(TILES)], axis=0
        )
        counts = dot(tiles.astype(BF16), earlier)
        for t in range(TILES):
            there = tiles[16 * t : 16 * t + 1] > 0.5
            where_from = tiles[16 * t + 1 : 16 * t + 2].astype(I32)
            columns[chip, core, s, t : t + 1, :] = jnp.where(there, where_from, PANEL)
        wide = jnp.concatenate([counts[16 * t : 16 * t + 16] for t in range(TILES)], axis=1)
        rank = dot(wide.astype(BF16), hot)[0:1].astype(I32)
        target = (glued // SHARE) * CAP + rank
        targets.append(target)

    def to_member(src, dst, send, recv, to):
        return pltpu.make_async_remote_copy(
            src_ref=src, dst_ref=dst, send_sem=send, recv_sem=recv,
            device_id=(cluster, to), device_id_type=MESH,
        )

    def chip_at(dx, dy):
        y, x = chip // SIDE, lax.rem(chip, SIDE)
        return lax.rem(y + dy, SIDE) * SIDE + lax.rem(x + dx, SIDE)

    def squares(s):
        live = sizes[s]
        found = []
        for i in range(STEPS):
            rows = pl.ds(i * STEP, STEP)
            square = factor[s, rows, rows]
            row_id, col_id = iota(square.shape, 0), iota(square.shape, 1)
            keep = (col_id <= row_id) & (row_id + i * STEP < live)
            found.append(jnp.where(keep, square, jnp.where(row_id == col_id, 1.0, 0.0)))
        return found

    def invert(s):
        for i in range(STEPS):
            factor_copy(s, i).wait()
        if s + 1 < SUBS:
            start_copies(s + 1)
        blocks = squares(s)
        for k in range(0, STEPS, BATCH):
            for i, found in enumerate(base_inverses(blocks[k : k + BATCH])):
                inverted[k + i] = found
        found = [inverted[i] for i in range(STEPS)]
        size = BASE
        while size < STEP:
            found = doubled(found, blocks, size)
            size *= 2
        for i in range(STEPS):
            half = split(found[i])
            step_high[s, i, 0:STEP], step_low[s, i, 0:STEP] = half
            if i < STEPS - 1:
                under = factor[s, pl.ds((i + 1) * STEP, STEP), pl.ds(i * STEP, STEP)]
                onward = split(dot3(split(under), half))
                step_high[s, i, STEP : 2 * STEP], step_low[s, i, STEP : 2 * STEP] = onward

    with jax.named_scope("invert"):
        invert(0)

    with jax.named_scope("barrier"):
        pl.semaphore_wait(barrier, MEMBERS + 1)

    def chip_at(dx, dy):
        y, x = chip // SIDE, lax.rem(chip, SIDE)
        return lax.rem(y + dy, SIDE) * SIDE + lax.rem(x + dx, SIDE)

    def along(first, second):
        return chip_at(
            first * (1 - core) + second * core, first * core + second * (1 - core)
        )

    def column_copy(origin, to):
        return to_member(
            columns.at[origin, core], columns.at[origin, core], column_send,
            column_recv.at[origin], to * CORES + core,
        )

    def load_copy(source, origin, to):
        return to_member(
            source, all_loads.at[origin, core], load_send, load_recv.at[origin], to * CORES + core
        )

    every = pl.ds(0, CHIPS)

    def pair_copy(ref, which, k):
        return to_member(
            ref.at[every, which], ref.at[every, which], pair_send.at[k], pair_recv.at[k], partner
        )

    with jax.named_scope("share"):
        for k in (1, 3, 2):
            load_copy(loads, chip, along(k, 0)).start()
            load_copy(loads, chip, along(0, k)).start()
        for dx, dy in AROUND:
            column_copy(chip, chip_at(dx, dy)).start()
        all_loads[chip, core] = loads[...]

    def substitute(s):
        live = sizes[s]
        panel_copy(s).wait()

        def masked(i, part):
            return jnp.where(iota(part.shape, 0) + i * STEP < live, part, 0.0)

        part = masked(0, rhs[s, 0:STEP, :])
        squared, cross = [], []
        for i in range(STEPS):
            halves = split(part)
            tall = STEP if i == STEPS - 1 else 2 * STEP
            both = dot3((step_high[s, i, 0:tall], step_low[s, i, 0:tall]), halves)
            if i < STEPS - 1:
                part = masked(i + 1, rhs[s, (i + 1) * STEP : (i + 2) * STEP, :] - both[STEP:])
            found = split(both[0:STEP])
            solved_high[i * STEP : (i + 1) * STEP], solved_low[i * STEP : (i + 1) * STEP] = found
            if i < STEPS - 2:
                rest = pl.ds((i + 2) * STEP, ORDER - (i + 2) * STEP)
                left = split(factor[s, rest, pl.ds(i * STEP, STEP)])
                rhs[s, rest, :] = rhs[s, rest, :] - dot3(left, found)
            if i % FOLD == FOLD - 1:
                done = pl.ds((i + 1 - FOLD) * STEP, FOLD * STEP)
                high = solved_high[done, :]
                squared.append(dot(high, high, ((0,), (0,))))
                cross.append(dot(high, solved_low[done, :], ((0,), (0,))))
        crossed = sum(cross[1:], cross[0])
        local = sum(squared[1:], squared[0]) + (crossed + crossed.T)
        local_high, local_low = split(local)
        picks = jnp.where(iota((MEMBERS * CAP, PANEL), 0) == targets[s], 1.0, 0.0).astype(BF16)
        values = dot(picks, local_high) + dot(picks, local_low)
        outgoing[s] = values.reshape(MEMBERS, CAP, PANEL)
        incoming[s, me] = outgoing[s, me]

    for s in range(SUBS):
        if s:
            with jax.named_scope("invert"):
                invert(1)

            with jax.named_scope("forward"):
                for first in (3, 1, 2):
                    origin = along(first, 0)
                    load_copy(loads, origin, origin).wait_recv()
                    for k in (1, 3, 2):
                        load_copy(all_loads.at[origin, core], origin, along(0, k)).start()

        with jax.named_scope("substitute"):
            substitute(s)

        if s:
            with jax.named_scope("gathered"):
                for dx, dy in AROUND:
                    origin = chip_at(dx, dy)
                    column_copy(origin, origin).wait_recv()
                pair_copy(columns, core, 0).start()

        def send(to):
            to_member(
                outgoing.at[s, to], incoming.at[s, me], value_send.at[s], value_recv.at[s, me], to
            ).start()

        with jax.named_scope("send"):

            @pl.loop(0, CORES)
            def _(dc):
                for dx, dy in AROUND:
                    send(chip_at(dx, dy) * CORES + lax.rem(core + dc, CORES))

            send(partner)

    with jax.named_scope("pair"):
        pair_copy(columns, 1 - core, 0).wait_recv()

    with jax.named_scope("ranks"):
        @pl.loop(0, MEMBERS)
        def _(m):
            for s in range(SUBS):
                tile = columns[m // CORES, lax.rem(m, CORES), s, pl.ds(me // (LANES // SHARE), 1), :]
                own_tile[pl.ds(s * MEMBERS + m, 1), :] = tile

        shift = lax.rem(me, LANES // SHARE) * SHARE
        own = own_tile[...]
        lane = iota(own.shape, 1)
        own = lanes_from(own, lax.rem(lane + shift, LANES))
        there = (own < PANEL) & (lane < SHARE)
        order = dot(jnp.where(there, 1.0, 0.0).astype(BF16), earlier).astype(I32)
        ranks[...] = jnp.where(there, order, -1)

    slot = iota((CAP, LANES), 0)
    stacked[...] = jnp.zeros_like(stacked)

    def place_one(s, source, k):
        rows = slice(k * CAP, (k + 1) * CAP)
        left = incoming[s, source, :, 0:LANES]
        right = incoming[s, source, :, LANES : 2 * LANES]
        source_chip, source_core = source // CORES, lax.rem(source, CORES)
        for t in range(TILES):
            index = jnp.broadcast_to(columns[source_chip, source_core, s, t : t + 1, :], (CAP, LANES))
            lane = index & (LANES - 1)
            value = jnp.where(index < LANES, lanes_from(left, lane), lanes_from(right, lane))
            value = jnp.where(index < PANEL, value, 0.0)
            high, low = split(value)
            spread_high[rows, t * LANES : (t + 1) * LANES] = high
            spread_low[rows, t * LANES : (t + 1) * LANES] = low
        here = jnp.where(slot == ranks[pl.ds(s * MEMBERS + source, 1), :], 1.0, 0.0)
        placing[rows, :] = here.astype(BF16)

    for s in range(SUBS):
        with jax.named_scope("place"):

            @pl.loop(0, CORES)
            def _(dc):
                if s:

                    @pl.when(dc == CORES - 1)
                    def _():
                        for second in (1, 3, 2):
                            for first in range(SIDE):
                                origin = along(first, second)
                                load_copy(loads, origin, origin).wait_recv()
                        pair_copy(all_loads, core, 1).start()

                for half in range(CHIPS // GROUP):
                    sources = [
                        chip_at((SIDE - dx) % SIDE, (SIDE - dy) % SIDE) * CORES
                        + lax.rem(core + dc, CORES)
                        for dx, dy in (AROUND + [(0, 0)])[half * GROUP : (half + 1) * GROUP]
                    ]

                    def wait(source):
                        to_member(
                            outgoing.at[s, 0], incoming.at[s, source], value_send.at[s],
                            value_recv.at[s, source], source,
                        ).wait_recv()

                    last = half == CHIPS // GROUP - 1
                    for source in sources[:-1] if last else sources:
                        wait(source)
                    if last:
                        pl.when(dc > 0)(functools.partial(wait, partner))
                    for k, source in enumerate(sources):
                        place_one(s, source, k)
                    place = placing[...]
                    part = dot(place, spread_high[...], ((0,), (0,))) + dot(
                        place, spread_low[...], ((0,), (0,))
                    )
                    part = part[0:SHARE]
                    stacked[...] = stacked[...] + part

    with jax.named_scope("apply"):
        pair_copy(all_loads, 1 - core, 1).wait_recv()
        owned = stacked[...]
        all_high, all_low = split(all_loads[...].reshape(NDUAL, PANEL))
        owned_high, owned_low = split(owned)
        product = dot(owned_high, all_high) + dot(owned_low, all_high) + dot(owned_high, all_low)
        raw[...] = product
        dual_out[...] = owned

    def end_copy(src, dst, k, to):
        return pltpu.make_async_remote_copy(
            src_ref=src, dst_ref=dst, send_sem=end_send.at[k], recv_sem=end_recv.at[k],
            device_id=(to, me), device_id_type=MESH,
        )

    up = end_copy(raw.at[pl.ds(SHARE - IFACE, IFACE)], before, 0, following)
    down = end_copy(raw.at[pl.ds(0, IFACE)], after, 1, preceding)
    with jax.named_scope("ends"):
        up.start()
        down.start()
        products_out[pl.ds(IFACE, SHARE - 2 * IFACE), :] = product[IFACE : SHARE - IFACE]
        up.wait()
        down.wait()
        products_out[pl.ds(0, IFACE), :] = product[0:IFACE] + before[...]
        products_out[pl.ds(SHARE - IFACE, IFACE), :] = product[SHARE - IFACE :] + after[...]

    others = pl.ds(0, MEMBERS - 1)
    with jax.named_scope("drain"):
        for s in range(SUBS):
            pltpu.make_async_copy(outgoing.at[s, others], incoming.at[s, others], value_send.at[s]).wait()
        far = pl.ds(0, CHIPS - 1)
        pltpu.make_async_copy(columns.at[far, 0], columns.at[far, 0], column_send).wait()
        pltpu.make_async_copy(all_loads.at[far, 0], all_loads.at[far, 0], load_send).wait()
        pair_copy(columns, core, 0).wait_send()
        pair_copy(all_loads, core, 1).wait_send()


def hand_over(owned, products, owned_out, products_out):
    owned_out[...] = owned[...]
    products_out[...] = products[...]


def on_device(factors, panels, sizes, glue_index, loads):
    vmem = pl.BlockSpec(memory_space=pltpu.VMEM)
    dma = pltpu.SemaphoreType.DMA
    owned, products = pl.pallas_call(
        kernel,
        out_shape=(
            jax.ShapeDtypeStruct((SHARE, NDUAL), F32),
            jax.ShapeDtypeStruct((SHARE, PANEL), F32),
        ),
        in_specs=[
            pl.BlockSpec(memory_space=pltpu.SMEM),
            pl.BlockSpec(memory_space=pl.ANY),
            pl.BlockSpec(memory_space=pl.ANY),
            vmem,
            vmem,
        ],
        out_specs=(vmem, vmem),
        scratch_shapes=[
            pltpu.VMEM((SUBS, ORDER, ORDER), F32),
            pltpu.VMEM((SUBS, ORDER, PANEL), F32),
            pltpu.VMEM((ORDER, PANEL), BF16),
            pltpu.VMEM((ORDER, PANEL), BF16),
            pltpu.VMEM((SUBS, STEPS, 2 * STEP, STEP), BF16),
            pltpu.VMEM((SUBS, STEPS, 2 * STEP, STEP), BF16),
            pltpu.VMEM((SUBS, MEMBERS, CAP, PANEL), F32),
            pltpu.VMEM((SUBS, MEMBERS, CAP, PANEL), F32),
            pltpu.VMEM((CHIPS, CORES, SUBS, TILES, LANES), I32),
            pltpu.VMEM((SUBS * MEMBERS, LANES), I32),
            pltpu.VMEM((SUBS * MEMBERS, LANES), I32),
            pltpu.VMEM((CHIPS, CORES, SHARE, PANEL), F32),
            pltpu.VMEM((STEPS, STEP, STEP), F32),
            pltpu.VMEM((GROUP * CAP, NDUAL), BF16),
            pltpu.VMEM((GROUP * CAP, NDUAL), BF16),
            pltpu.VMEM((GROUP * CAP, LANES), BF16),
            pltpu.VMEM((SHARE, NDUAL), F32),
            pltpu.VMEM((SHARE, PANEL), F32),
            pltpu.VMEM((IFACE, PANEL), F32),
            pltpu.VMEM((IFACE, PANEL), F32),
            dma((SUBS, STEPS)),
            dma((SUBS,)),
            dma((SUBS,)),
            dma((SUBS, MEMBERS)),
            dma,
            dma((CHIPS,)),
            dma,
            dma((CHIPS,)),
            dma((2,)),
            dma((2,)),
            dma((2,)),
            dma((2,)),
        ],
        compiler_params=pltpu.CompilerParams(
            collective_id=0, has_side_effects=True, vmem_limit_bytes=56 * 2**20
        ),
        name="dual_operator",
    )(sizes, factors, panels, glue_index, loads)
    return pl.pallas_call(
        hand_over,
        out_shape=(
            jax.ShapeDtypeStruct((SHARE, NDUAL), F32),
            jax.ShapeDtypeStruct((SHARE, PANEL), F32),
        ),
        in_specs=[vmem, vmem],
        out_specs=(vmem, vmem),
        name="hand_over",
    )(owned, products)


def solution(mesh):
    whole = ("cluster", "member")
    return jax.shard_map(
        on_device,
        mesh=mesh,
        in_specs=(P(whole, None, None), P(whole, None, None), P(whole), P(whole, None), P(whole, None)),
        out_specs=(P(whole, None), P(whole, None)),
        check_vma=False,
    )
```
